128 devices in a mesh: sims: 4 (over x_lo, core), ell: 32 (over x_hi, z, y).
Axes of the slice: x: 4 (x_hi: 2, x_lo: 2; x = x_hi * 2 + x_lo), y: 4, z: 4, core: 2. Of those that a mesh axis runs over, the one named last changes fastest.
Arguments:
- spectra: float32 [3, 6144, 896], P(None, 'ell', 'sims'), parts along dimension 2, may hold values from -6 to 6
- tables: float32 [3, 6144, 6144], P(None, 'ell'), may hold values from -0.15625 to 0.15625
- apodization: float32 [6144], replicated, may hold values from 0.2 to 1
- inv_mask: float32 [6144], replicated, may hold values from 0.5 to 4
- weights: float32 [6144], replicated, may hold values from 0.5 to 1.5
Outputs:
- corrected: float32 [3, 6144, 896], P(None, 'ell', 'sims'), parts along dimension 2
The draws below stay inside these ranges and needn't reach their ends.
There are 4 independent parts, one for each index of `sims`. The reference program is written for one: setup_inputs(seed, part) draws one part's arguments, and reference() takes and returns one part's arrays. A program takes and returns all parts, laid end to end along the dimension named above; an argument that names none is the same for every part. Nothing has to cross between parts.
All inputs are finite; a program needn't handle non-finite values.
Results may differ from the reference program's by a relative error of at most 0.000094.
Values sent between devices are 32-bit elements; how exact they have to be, the bound alone decides.
A program may use at most 128 MiB of HBM per device.

```python
import math
import jax
import jax.numpy as jnp
from jax import lax

L = 6144
A = 6144
NSIM = 224


def strengthened(entries, key, source, target, parts, factor):
    def block_of(dim):
        return (jnp.arange(entries.shape[dim]) // (entries.shape[dim] // parts)).reshape((-1,) + (1,) * (entries.ndim - 1 - dim))

    first = jax.random.permutation(key, parts)[block_of(target)]
    other_side = (block_of(target) + parts // 2) % parts
    return jnp.where((block_of(source) == first) | (block_of(source) == other_side), factor * entries, entries)


def levels(key, extent, cuts, low, top_value):
    level = 1.0
    for position, shards_of in cuts:
        steps = jax.random.uniform(jax.random.fold_in(jax.random.fold_in(key, 6), position), (shards_of,), jnp.float32, low / len(cuts), top_value / len(cuts))
        level = level * jnp.repeat(jnp.exp(steps), extent[position] // shards_of).reshape((-1,) + (1,) * (len(extent) - 1 - position))
    return level


def gaussian(rng, extent, spread, bound, pieces=(), held_as=jnp.bfloat16):
    entries = spread * jax.random.normal(rng, extent, jnp.float32)
    if pieces:
        entries = entries * levels(rng, extent, pieces, -0.22, 0.18)
    return jnp.clip(entries, -bound, bound).astype(held_as)


def bell_draw_with(own_key, shape, scale, most, cuts, heavy, kind=jnp.bfloat16):
    entries = scale * jax.random.normal(own_key, shape, jnp.float32)
    if cuts:
        entries = entries * levels(own_key, shape, cuts, -0.22, 0.18)
    return jnp.clip(strengthened(entries, jax.random.fold_in(own_key, 3), *heavy), -most, most).astype(kind)


def setup_inputs(seed: int = 0, part: int = 0) -> dict:
    key_list = jax.random.split(jax.random.key(seed), 6)
    part_keys = jax.random.split(jax.random.fold_in(key_list[5], part), 6)
    spectra = gaussian(part_keys[0], (3, L, NSIM), 1.0, 6.0, ((1, 32),), jnp.float32)
    tables = bell_draw_with(key_list[1], (3, L, A), L ** -0.5, 0.15625, ((1, 32),), (1, 2, 32, 2.75), jnp.float32)
    apodization = jnp.clip(jax.random.uniform(key_list[2], (A,), jnp.float32, 0.2, 1.0), 0.2, 1.0)
    inv_mask = jnp.clip(jnp.exp(jax.random.uniform(key_list[3], (A,), jnp.float32, math.log(0.5), math.log(4.0))), 0.5, 4.0)
    weights = jnp.clip(jax.random.uniform(key_list[4], (A,), jnp.float32, 0.5, 1.5), 0.5, 1.5)
    return {"spectra": spectra, "tables": tables, "apodization": apodization, "inv_mask": inv_mask, "weights": weights}


def reference(spectra, tables, apodization, inv_mask, weights):
    highest = lax.Precision.HIGHEST
    combined = jnp.stack([spectra[0], spectra[1] + spectra[2], spectra[1] - spectra[2]])
    corr = jnp.einsum('pla,pls->aps', tables, combined, precision=highest)
    factor = weights * apodization * inv_mask
    fixed = corr * factor[:, None, None]
    back = jnp.einsum('pla,aps->pls', tables, fixed, precision=highest)
    return jnp.stack([back[0], 0.5 * (back[1] + back[2]), 0.5 * (back[1] - back[2])])
```

```python
import jax
import jax.numpy as jnp
from jax import lax
from jax.sharding import PartitionSpec as P

CHUNKS = 1
PRECISION = lax.Precision.HIGH


def ell_perm(dx, dz, dy):
    pairs = []
    for e in range(32):
        x, z, y = e // 16, e // 4 % 4, e % 4
        pairs.append((e, ((x + dx) % 2 * 4 + (z + dz) % 4) * 4 + (y + dy) % 4))
    return pairs


def shift_y(v, d):
    return lax.ppermute(v, "ell", ell_perm(0, 0, d))


def shift_z(v, d):
    return lax.ppermute(v, "ell", ell_perm(0, d, 0))


def swap_x_hi(v):
    return lax.ppermute(v, "ell", ell_perm(1, 0, 0))


def swap_sims(v, mask):
    return lax.ppermute(v, "sims", [(s, s ^ mask) for s in range(4)])


def rows_of(v, start, count):
    return lax.dynamic_slice_in_dim(v, start, count, 0)


def gather_y(own):
    half = own.shape[0] // 2
    below = shift_y(own, 1)
    above = shift_y(own, -1)
    far = jnp.concatenate([shift_y(below[:half], 1), shift_y(above[half:], -1)])
    return below, above, far


def local(spectra, tables, apodization, inv_mask, weights):
    sims, ell = lax.axis_index("sims"), lax.axis_index("ell")
    y, z = ell % 4, ell // 4 % 4
    _, depth, angles = tables.shape
    nsim = spectra.shape[2]
    span = angles // 4
    width = span // CHUNKS
    quarter, eighth = depth // 4, depth // 8
    part = nsim // 4
    factor = weights * apodization * inv_mask
    combined = [spectra[0], spectra[1] + spectra[2], spectra[1] - spectra[2]]
    order = [sims, sims ^ 2, sims ^ 1, sims ^ 3]

    def table_chunk(p, h):
        def cut(row, count, d):
            return lax.dynamic_slice(
                tables[p], (row, (y + d) % 4 * span + h * width), (count, width)
            )

        mine = sims * quarter
        below = shift_y(
            jnp.concatenate([cut(mine, quarter, 1), cut(mine, eighth, 2)]), 1
        )
        above = shift_y(
            jnp.concatenate([cut(mine, quarter, 3), cut(mine + eighth, eighth, 2)]), -1
        )
        far_low = shift_y(below[quarter:], 1)
        far_high = shift_y(above[quarter:], -1)
        held = jnp.concatenate([below[:quarter], above[:quarter], far_low, far_high])
        across = swap_sims(held, 2)
        return jnp.concatenate(
            [cut(0, depth, 0), held, across, swap_sims(held, 1), swap_sims(across, 1)]
        )

    def reduce_z(corr):
        half = corr.shape[1] // 2

        def block(d):
            return rows_of(corr, (z + d) % 4 * part, part)

        far = block(2)
        low = shift_z(far[:, :half], 1)
        high = shift_z(far[:, half:], -1)
        up, down = block(1), block(3)
        up = jnp.concatenate([up[:, :half] + low, up[:, half:]], 1)
        down = jnp.concatenate([down[:, :half], down[:, half:] + high], 1)
        total = block(0) + shift_z(up, 1) + shift_z(down, -1)
        return total + swap_x_hi(total)

    def gather_z(own):
        half = own.shape[1] // 2
        below = shift_z(own, 1)
        above = shift_z(own, -1)
        far = jnp.concatenate(
            [shift_z(below[:, :half], 1), shift_z(above[:, half:], -1)], 1
        )
        full = jnp.zeros((nsim, own.shape[1]), own.dtype)
        for d, v in ((0, own), (3, below), (1, above), (2, far)):
            full = lax.dynamic_update_slice_in_dim(full, v, (z + d) % 4 * part, 0)
        return full

    outs = []
    for p in range(3):
        blocks = gather_y(combined[p])
        coeffs = jnp.concatenate(
            [combined[p]]
            + [rows_of(b, q * quarter, quarter) for q in order for b in blocks]
        )
        back = None
        for h in range(CHUNKS):
            table = table_chunk(p, h)
            corr = lax.dot_general(
                coeffs, table, (((0,), (0,)), ((), ())), precision=PRECISION
            )
            scale = lax.dynamic_slice_in_dim(factor, y * span + h * width, width)
            fixed = gather_z(reduce_z(corr) * scale)
            term = lax.dot_general(
                table, fixed, (((1,), (1,)), ((), ())), precision=PRECISION
            )
            back = term if back is None else back + term
        half = depth // 2
        rest = back[depth:].reshape(4, 3, quarter, nsim)

        def owner(j):
            flipped = [rest[k, j] for k in (0, 2, 1, 3)]
            s1 = (sims & 1) == 1
            s2 = (sims & 2) == 2
            a = [jnp.where(s1, flipped[k ^ 1], flipped[k]) for k in range(4)]
            return jnp.concatenate([jnp.where(s2, a[k ^ 2], a[k]) for k in range(4)])

        to_below, to_above, to_far = owner(0), owner(1), owner(2)
        low = shift_y(to_far[:half], 1)
        high = shift_y(to_far[half:], -1)
        up = jnp.concatenate([to_above[:half] + low, to_above[half:]])
        down = jnp.concatenate([to_below[:half], to_below[half:] + high])
        outs.append(back[:depth] + shift_y(up, 1) + shift_y(down, -1))
    return jnp.stack([outs[0], 0.5 * (outs[1] + outs[2]), 0.5 * (outs[1] - outs[2])])


def solution(mesh):
    placed = (P(None, "ell", "sims"), P(None, "ell", None), P(), P(), P())
    return jax.shard_map(
        local, mesh=mesh, in_specs=placed, out_specs=P(None, "ell", "sims"), check_vma=False
    )
```

```python
import jax
import jax.numpy as jnp
from jax import lax
from jax.experimental import pallas as pl
from jax.experimental.pallas import tpu as pltpu
from jax.sharding import PartitionSpec as P

WIDTH = 256
SLOTS = 4
DELAY = dict(relay=1, share=2, pass_on=3, corr=4, fold=5, total=6, scale=7,
             spread=8, back=9, ret=10, ret_fold=11, ret_sum=12)
F32, BF16 = jnp.float32, jnp.bfloat16


def split(x):
    high = x.astype(BF16)
    return high, (x - high.astype(F32)).astype(BF16)


def dot3(a, b, dims):
    def dot(u, v):
        return lax.dot_general(u, v, (dims, ((), ())), preferred_element_type=F32)

    return dot(a[0], b[0]) + (dot(a[0], b[1]) + dot(a[1], b[0]))


def kernel(spec, tables, weights, apod, inv_mask, out, tbl, relay, coef, corr, near,
           part, other, tot, fixed, back, ret1, ret2, own_sem, send, recv, p_send, p_recv):
    sims, ell = lax.axis_index("sims"), lax.axis_index("ell")
    y, z, x = lax.rem(ell, 4), lax.rem(lax.div(ell, 4), 4), lax.div(ell, 16)
    depth, nsim = out.shape[1], out.shape[2]
    span = tbl.shape[3]
    per = span // WIDTH
    chunks = 3 * per
    quarter, eighth = depth // 4, depth // 8
    group = nsim // 4
    half_w, half_d, half_s = WIDTH // 2, depth // 2, nsim // 2

    def ring(v, d):
        return lax.rem(v + d, 4)

    def at_y(d):
        return (sims, (x * 4 + z) * 4 + ring(y, d))

    def at_z(d):
        return (sims, (x * 4 + ring(z, d)) * 4 + y)

    y_up, y_down, z_up, z_down = at_y(1), at_y(3), at_z(1), at_z(3)
    x_peer = (sims, ((1 - x) * 4 + z) * 4 + y)
    flip1 = sims + 1 - 2 * lax.rem(sims, 2)
    flip2 = lax.rem(sims + 2, 4)
    core, x_near = (flip1, ell), (flip2, ell)

    def aligned(v, m):
        return pl.multiple_of(v, m)

    def z_rows(d):
        return pl.ds(aligned(ring(z, d) * group, 8), group)

    def start(kind, c, src, dst, device):
        copy = pltpu.make_async_remote_copy(
            src, dst, send.at[kind, lax.rem(c, SLOTS)], recv.at[kind, c],
            device_id=device, device_id_type=pl.DeviceIdType.MESH)

        @pl.when(c >= SLOTS)
        def _():
            copy.wait_send()

        copy.start()

    def arrived(kind, c, ref):
        pltpu.make_async_copy(ref, ref, recv.at[kind, c]).wait()

    def start_p(kind, p, src, dst, device):
        pltpu.make_async_remote_copy(
            src, dst, p_send.at[kind, p], p_recv.at[kind, p],
            device_id=device, device_id_type=pl.DeviceIdType.MESH).start()

    def arrived_p(kind, p, ref):
        pltpu.make_async_copy(ref, ref, p_recv.at[kind, p]).wait()

    def sent_p(kind, p, ref):
        pltpu.make_async_copy(ref, ref, p_send.at[kind, p]).wait()

    def where(c):
        p = lax.div(c, per)
        h = c - p * per
        return p, h, pl.ds(aligned(h * WIDTH, WIDTH), WIDTH)

    q0 = aligned(sims * quarter, 8)
    mine = pl.ds(q0, quarter)
    low_rows = pl.ds(q0, eighth)
    high_rows = pl.ds(aligned(q0 + eighth, 8), eighth)
    near_rows = pl.ds(aligned(flip2 * quarter, 8), quarter)
    core_rows = pl.ds(aligned(flip1 * quarter, 8), quarter)
    last_rows = pl.ds(aligned(lax.rem(flip1 + 2, 4) * quarter, 8), quarter)
    others = pl.ds(1, 3)

    def stage_send(c):
        p, h, cols = where(c)

        def source(rows, d):
            return tables.at[p, rows, pl.ds(aligned(ring(y, d) * span + h * WIDTH, WIDTH), WIDTH)]

        start(2, c, source(low_rows, 2), relay.at[0, c], y_up)
        start(3, c, source(high_rows, 2), relay.at[1, c], y_down)
        start(0, c, source(mine, 1), tbl.at[p, 1, mine, cols], y_up)
        start(1, c, source(mine, 3), tbl.at[p, 2, mine, cols], y_down)

    def stage_relay(c):
        p, h, cols = where(c)
        arrived(2, c, relay.at[0, c])
        start(4, c, relay.at[0, c], tbl.at[p, 3, low_rows, cols], y_up)
        arrived(3, c, relay.at[1, c])
        start(5, c, relay.at[1, c], tbl.at[p, 3, high_rows, cols], y_down)

    def stage_share(c):
        p, h, cols = where(c)
        arrived(0, c, tbl.at[p, 1, mine, cols])
        arrived(1, c, tbl.at[p, 2, mine, cols])
        arrived(4, c, tbl.at[p, 3, low_rows, cols])
        arrived(5, c, tbl.at[p, 3, high_rows, cols])
        block = tbl.at[p, others, mine, cols]
        start(6, c, block, block, x_near)
        start(7, c, block, block, core)

    def stage_pass_on(c):
        p, h, cols = where(c)
        block = tbl.at[p, others, near_rows, cols]
        arrived(6, c, block)
        start(8, c, block, block, core)

    def stage_corr(c):
        p, h, cols = where(c)
        arrived(7, c, tbl.at[p, others, core_rows, cols])
        arrived(8, c, tbl.at[p, others, last_rows, cols])

        @pl.when(h == 0)
        def _():
            pltpu.make_async_copy(tbl.at[p, 0], tbl.at[p, 0], own_sem.at[0, p]).wait()
            pltpu.make_async_copy(coef.at[p, 0], coef.at[p, 0], own_sem.at[1, p]).wait()
            arrived_p(6, p, coef.at[p, 3, pl.ds(0, half_s)])
            arrived_p(7, p, coef.at[p, 3, pl.ds(half_s, half_s)])

        total = dot3(split(coef[p, 0]), split(tbl[p, 0, :, cols]), ((1,), (0,)))
        for r in range(1, 4):
            total += dot3(split(coef[p, r]), split(tbl[p, r, :, cols]), ((1,), (0,)))
        corr[c] = total
        far = z_rows(2)
        start(9, c, corr.at[c, far, pl.ds(0, half_w)], near.at[c, 0], z_up)
        start(10, c, corr.at[c, far, pl.ds(half_w, half_w)], near.at[c, 1], z_down)

    def stage_fold(c):
        up, down = z_rows(1), z_rows(3)
        arrived(9, c, near.at[c, 0])
        corr[c, up, pl.ds(0, half_w)] += near[c, 0]
        start(11, c, corr.at[c, up], part.at[c, 0], z_up)
        arrived(10, c, near.at[c, 1])
        corr[c, down, pl.ds(half_w, half_w)] += near[c, 1]
        start(12, c, corr.at[c, down], part.at[c, 1], z_down)

    def stage_total(c):
        arrived(11, c, part.at[c, 0])
        arrived(12, c, part.at[c, 1])
        tot[c] = corr[c, z_rows(0)] + (part[c, 0] + part[c, 1])
        start(13, c, tot.at[c], other.at[c], x_peer)

    def stage_scale(c):
        p, h, cols = where(c)
        arrived(13, c, other.at[c])
        row = pl.ds(y * per + h, 1)
        factor = weights[row, :] * apod[row, :] * inv_mask[row, :]
        rows = z_rows(0)
        fixed[c, rows] = (tot[c] + other[c]) * factor
        start(14, c, fixed.at[c, rows], fixed.at[c, rows], z_up)
        start(15, c, fixed.at[c, rows], fixed.at[c, rows], z_down)

    def stage_spread(c):
        below = fixed.at[c, z_rows(3), pl.ds(0, half_w)]
        above = fixed.at[c, z_rows(1), pl.ds(half_w, half_w)]
        arrived(14, c, fixed.at[c, z_rows(3)])
        start(16, c, below, below, z_up)
        arrived(15, c, fixed.at[c, z_rows(1)])
        start(17, c, above, above, z_down)

    def stage_back(c):
        p, h, cols = where(c)
        arrived(16, c, fixed.at[c, z_rows(2), pl.ds(0, half_w)])
        arrived(17, c, fixed.at[c, z_rows(2), pl.ds(half_w, half_w)])
        values = split(fixed[c])
        for r in range(4):
            back[p, r] += dot3(split(tbl[p, r, :, cols]), values, ((1,), (1,)))

    top, bottom = pl.ds(0, half_d), pl.ds(half_d, half_d)

    def ends(c):
        p = lax.div(c, per)
        return p, c - p * per == per - 1

    def stage_ret(c):
        p, last = ends(c)

        @pl.when(last)
        def _():
            start_p(0, p, back.at[p, 3, top], ret1.at[p, 0], y_up)
            start_p(1, p, back.at[p, 3, bottom], ret1.at[p, 1], y_down)

    def stage_ret_fold(c):
        p, last = ends(c)

        @pl.when(last)
        def _():
            arrived_p(0, p, ret1.at[p, 0])
            back[p, 2, top] += ret1[p, 0]
            start_p(2, p, back.at[p, 2], ret2.at[p, 0], y_up)
            arrived_p(1, p, ret1.at[p, 1])
            back[p, 1, bottom] += ret1[p, 1]
            start_p(3, p, back.at[p, 1], ret2.at[p, 1], y_down)

    def stage_ret_sum(c):
        p, last = ends(c)

        @pl.when(last)
        def _():
            arrived_p(2, p, ret2.at[p, 0])
            arrived_p(3, p, ret2.at[p, 1])
            back[p, 0] += ret2[p, 0] + ret2[p, 1]

    def coef_send(p):
        start_p(4, p, spec.at[p], coef.at[p, 1], y_up)
        start_p(5, p, spec.at[p], coef.at[p, 2], y_down)

    def coef_relay(p):
        first, second = pl.ds(0, half_s), pl.ds(half_s, half_s)
        arrived_p(4, p, coef.at[p, 1])
        start_p(6, p, coef.at[p, 1, first], coef.at[p, 3, first], y_up)
        arrived_p(5, p, coef.at[p, 2])
        start_p(7, p, coef.at[p, 2, second], coef.at[p, 3, second], y_down)

    for p in range(3):
        pltpu.make_async_copy(
            tables.at[p, :, pl.ds(aligned(y * span, WIDTH), span)], tbl.at[p, 0], own_sem.at[0, p]).start()
        pltpu.make_async_copy(spec.at[p], coef.at[p, 0], own_sem.at[1, p]).start()

    peers = (y_up, y_down, z_up, z_down, x_peer, x_near, core)
    barrier = pltpu.get_barrier_semaphore()
    for peer in peers:
        pl.semaphore_signal(barrier, inc=1, device_id=peer, device_id_type=pl.DeviceIdType.MESH)
    pl.semaphore_wait(barrier, len(peers))

    coef_send(0)
    stage_send(0)
    back[...] = jnp.zeros_like(back)
    coef_relay(0)

    stages = dict(relay=stage_relay, share=stage_share, pass_on=stage_pass_on,
                  fold=stage_fold, total=stage_total, scale=stage_scale, spread=stage_spread,
                  corr=stage_corr, back=stage_back, ret=stage_ret,
                  ret_fold=stage_ret_fold, ret_sum=stage_ret_sum)

    def tick(t, carry):
        @pl.when(t < chunks - 1)
        def _():
            stage_send(t + 1)

        for p in (1, 2):
            @pl.when(t == p * per - 4)
            def _():
                coef_send(p)

            @pl.when(t == p * per - 2)
            def _():
                coef_relay(p)

        for name, stage in stages.items():
            c = t - (DELAY[name] - 1)

            @pl.when((c >= 0) & (c < chunks))
            def _():
                stage(c)

        return carry

    lax.fori_loop(0, chunks + DELAY["ret_sum"] - 1, tick, 0)

    out[0] = back[0, 0]
    out[1] = 0.5 * (back[1, 0] + back[2, 0])
    out[2] = 0.5 * (back[1, 0] - back[2, 0])

    def drain(i, carry):
        def sent(kind, ref):
            pltpu.make_async_copy(ref, ref, send.at[kind, i]).wait()

        quarter_block = tbl.at[0, 0, pl.ds(0, quarter), pl.ds(0, WIDTH)]
        eighth_block = tbl.at[0, 0, pl.ds(0, eighth), pl.ds(0, WIDTH)]
        three_blocks = tbl.at[0, others, pl.ds(0, quarter), pl.ds(0, WIDTH)]
        group_block = fixed.at[0, pl.ds(0, group)]
        half_block = fixed.at[0, pl.ds(0, group), pl.ds(0, half_w)]
        shapes = ([quarter_block] * 2 + [eighth_block] * 4 + [three_blocks] * 3
                  + [half_block] * 2 + [group_block] * 5 + [half_block] * 2)
        for kind, ref in enumerate(shapes):
            sent(kind, ref)
        return carry

    lax.fori_loop(0, SLOTS, drain, 0)

    def drain_p(p, carry):
        sent_p(0, p, ret1.at[p, 0])
        sent_p(1, p, ret1.at[p, 1])
        sent_p(2, p, ret2.at[p, 0])
        sent_p(3, p, ret2.at[p, 1])
        sent_p(4, p, coef.at[p, 1])
        sent_p(5, p, coef.at[p, 2])
        sent_p(6, p, coef.at[p, 3, pl.ds(0, half_s)])
        sent_p(7, p, coef.at[p, 3, pl.ds(half_s, half_s)])
        return carry

    lax.fori_loop(0, 3, drain_p, 0)


def local(spectra, tables, apodization, inv_mask, weights):
    _, depth, angles = tables.shape
    nsim = spectra.shape[2]
    span, group = angles // 4, nsim // 4
    chunks = 3 * span // WIDTH
    combined = jnp.stack([spectra[0], spectra[1] + spectra[2], spectra[1] - spectra[2]])
    turned = jnp.swapaxes(combined, 1, 2)
    rows = [v.reshape(-1, WIDTH) for v in (weights, apodization, inv_mask)]
    vmem = pl.BlockSpec(memory_space=pltpu.VMEM)
    hbm = pl.BlockSpec(memory_space=pl.ANY)

    def buffer(*shape):
        return pltpu.VMEM(shape, F32)

    return pl.pallas_call(
        kernel,
        out_shape=jax.ShapeDtypeStruct(spectra.shape, F32),
        in_specs=[hbm, hbm, vmem, vmem, vmem],
        out_specs=vmem,
        scratch_shapes=[
            buffer(3, 4, depth, span),
            buffer(2, chunks, depth // 8, WIDTH),
            buffer(3, 4, nsim, depth),
            buffer(chunks, nsim, WIDTH),
            buffer(chunks, 2, group, WIDTH // 2),
            buffer(chunks, 2, group, WIDTH),
            buffer(chunks, group, WIDTH),
            buffer(chunks, group, WIDTH),
            buffer(chunks, nsim, WIDTH),
            buffer(3, 4, depth, nsim),
            buffer(3, 2, depth // 2, nsim),
            buffer(3, 2, depth, nsim),
            pltpu.SemaphoreType.DMA((2, 3)),
            pltpu.SemaphoreType.DMA((18, SLOTS)),
            pltpu.SemaphoreType.DMA((18, chunks)),
            pltpu.SemaphoreType.DMA((8, 3)),
            pltpu.SemaphoreType.DMA((8, 3)),
        ],
        compiler_params=pltpu.CompilerParams(
            collective_id=0, has_side_effects=True, vmem_limit_bytes=60 * 1024 * 1024),
    )(turned, tables, *rows)


def solution(mesh):
    placed = (P(None, "ell", "sims"), P(None, "ell", None), P(), P(), P())
    return jax.shard_map(
        local, mesh=mesh, in_specs=placed, out_specs=P(None, "ell", "sims"), check_vma=False
    )
```

```python
import jax
import jax.numpy as jnp
from jax import lax
from jax.experimental import pallas as pl
from jax.experimental.pallas import tpu as pltpu
from jax.sharding import PartitionSpec as P

WIDTH = 256
SLOTS = 4
ORDER = ("back", "corr", "fold", "relay", "ret", "pass_on", "ret_fold", "ret_sum", "total",
         "spread", "scale", "share", "send")
LEAD, FIRST = 2, 1
DELAY = dict(send=-LEAD, relay=0, share=1, pass_on=3, corr=4, fold=5, total=6, scale=8,
             spread=10, back=13, ret=13, ret_fold=15, ret_sum=17)
F32, BF16 = jnp.float32, jnp.bfloat16


def split(x):
    high = x.astype(BF16)
    return high, (x - high.astype(F32)).astype(BF16)


def dot3(a, b, dims):
    def dot(u, v):
        return lax.dot_general(u, v, (dims, ((), ())), preferred_element_type=F32)

    return dot(a[0], b[0]) + (dot(a[0], b[1]) + dot(a[1], b[0]))


def kernel(spec, tables, weights, apod, inv_mask, out, tbl, relay, coef, coef_hi, coef_lo, corr,
           near, part, other, tot, fixed, back, ret1, ret2, own_sem, send, recv, p_send, p_recv):
    sims, ell = lax.axis_index("sims"), lax.axis_index("ell")
    y, z, x = lax.rem(ell, 4), lax.rem(lax.div(ell, 4), 4), lax.div(ell, 16)
    depth, nsim = out.shape[1], out.shape[2]
    span = tbl.shape[3]
    per = span // WIDTH
    chunks = 3 * per
    quarter, eighth = depth // 4, depth // 8
    group = nsim // 4
    half_w, half_d = WIDTH // 2, depth // 2

    def ring(v, d):
        return lax.rem(v + d, 4)

    def at_y(d):
        return (sims, (x * 4 + z) * 4 + ring(y, d))

    def at_z(d):
        return (sims, (x * 4 + ring(z, d)) * 4 + y)

    y_up, y_down, z_up, z_down = at_y(1), at_y(3), at_z(1), at_z(3)
    x_peer = (sims, ((1 - x) * 4 + z) * 4 + y)
    flip1 = sims + 1 - 2 * lax.rem(sims, 2)
    flip2 = lax.rem(sims + 2, 4)
    core, x_near = (flip1, ell), (flip2, ell)

    def aligned(v, m):
        return pl.multiple_of(v, m)

    def z_rows(d):
        return pl.ds(aligned(ring(z, d) * group, 8), group)

    def start(kind, c, src, dst, device):
        copy = pltpu.make_async_remote_copy(
            src, dst, send.at[kind, lax.rem(c, SLOTS)], recv.at[kind, c],
            device_id=device, device_id_type=pl.DeviceIdType.MESH)

        @pl.when(c >= SLOTS)
        def _():
            copy.wait_send()

        copy.start()

    def arrived(kind, c, ref):
        pltpu.make_async_copy(ref, ref, recv.at[kind, c]).wait()

    def start_p(kind, p, src, dst, device):
        pltpu.make_async_remote_copy(
            src, dst, p_send.at[kind, p], p_recv.at[kind, p],
            device_id=device, device_id_type=pl.DeviceIdType.MESH).start()

    def arrived_p(kind, p, ref):
        pltpu.make_async_copy(ref, ref, p_recv.at[kind, p]).wait()

    def sent_p(kind, p, ref):
        pltpu.make_async_copy(ref, ref, p_send.at[kind, p]).wait()

    def where(c):
        p = lax.div(c, per)
        h = c - p * per
        return p, h, pl.ds(aligned(h * WIDTH, WIDTH), WIDTH)

    q0 = aligned(sims * quarter, 8)
    mine = pl.ds(q0, quarter)
    low_rows = pl.ds(q0, eighth)
    high_rows = pl.ds(aligned(q0 + eighth, 8), eighth)
    near_rows = pl.ds(aligned(flip2 * quarter, 8), quarter)
    core_rows = pl.ds(aligned(flip1 * quarter, 8), quarter)
    last_rows = pl.ds(aligned(lax.rem(flip1 + 2, 4) * quarter, 8), quarter)
    others = pl.ds(1, 3)
    top, bottom = pl.ds(0, half_d), pl.ds(half_d, half_d)

    def stage_send(c):
        p, h, cols = where(c)

        def source(rows, d):
            return tables.at[p, rows, pl.ds(aligned(ring(y, d) * span + h * WIDTH, WIDTH), WIDTH)]

        start(2, c, source(low_rows, 2), relay.at[0, c], y_up)
        start(3, c, source(high_rows, 2), relay.at[1, c], y_down)
        start(0, c, source(mine, 1), tbl.at[p, 1, mine, cols], y_up)
        start(1, c, source(mine, 3), tbl.at[p, 2, mine, cols], y_down)

    def stage_relay(c):
        p, h, cols = where(c)
        arrived(2, c, relay.at[0, c])
        start(4, c, relay.at[0, c], tbl.at[p, 3, low_rows, cols], y_up)
        arrived(3, c, relay.at[1, c])
        start(5, c, relay.at[1, c], tbl.at[p, 3, high_rows, cols], y_down)

    def stage_share(c):
        p, h, cols = where(c)
        arrived(0, c, tbl.at[p, 1, mine, cols])
        arrived(1, c, tbl.at[p, 2, mine, cols])
        arrived(4, c, tbl.at[p, 3, low_rows, cols])
        arrived(5, c, tbl.at[p, 3, high_rows, cols])
        block = tbl.at[p, others, mine, cols]
        start(6, c, block, block, x_near)
        start(7, c, block, block, core)

    def stage_pass_on(c):
        p, h, cols = where(c)
        block = tbl.at[p, others, near_rows, cols]
        arrived(6, c, block)
        start(8, c, block, block, core)

    def stage_corr(c):
        p, h, cols = where(c)
        arrived(7, c, tbl.at[p, others, core_rows, cols])
        arrived(8, c, tbl.at[p, others, last_rows, cols])

        @pl.when(h == 0)
        def _():
            pltpu.make_async_copy(tbl.at[p, 0], tbl.at[p, 0], own_sem.at[0, p]).wait()
            arrived_p(6, p, coef.at[p, 3, top])
            arrived_p(7, p, coef.at[p, 3, bottom])
            for r in range(4):
                coef_hi[r], coef_lo[r] = split(coef[p, r].T)

        total = dot3((coef_hi[0], coef_lo[0]), split(tbl[p, 0, :, cols]), ((1,), (0,)))
        for r in range(1, 4):
            total += dot3((coef_hi[r], coef_lo[r]), split(tbl[p, r, :, cols]), ((1,), (0,)))
        corr[c] = total
        far = z_rows(2)
        start(9, c, corr.at[c, far, pl.ds(0, half_w)], near.at[c, 0], z_up)
        start(10, c, corr.at[c, far, pl.ds(half_w, half_w)], near.at[c, 1], z_down)

    def stage_fold(c):
        up, down = z_rows(1), z_rows(3)
        arrived(9, c, near.at[c, 0])
        corr[c, up, pl.ds(0, half_w)] += near[c, 0]
        start(11, c, corr.at[c, up], part.at[c, 0], z_up)
        arrived(10, c, near.at[c, 1])
        corr[c, down, pl.ds(half_w, half_w)] += near[c, 1]
        start(12, c, corr.at[c, down], part.at[c, 1], z_down)

    def stage_total(c):
        arrived(11, c, part.at[c, 0])
        arrived(12, c, part.at[c, 1])
        tot[c] = corr[c, z_rows(0)] + (part[c, 0] + part[c, 1])
        start(13, c, tot.at[c], other.at[c], x_peer)

    def stage_scale(c):
        p, h, cols = where(c)
        arrived(13, c, other.at[c])
        here = pl.ds(aligned(y * span + h * WIDTH, WIDTH), WIDTH)
        factor = weights[:, here] * apod[:, here] * inv_mask[:, here]
        rows = z_rows(0)
        fixed[c, rows] = (tot[c] + other[c]) * factor
        start(14, c, fixed.at[c, rows], fixed.at[c, rows], z_up)
        start(15, c, fixed.at[c, rows], fixed.at[c, rows], z_down)

    def stage_spread(c):
        below = fixed.at[c, z_rows(3), pl.ds(0, half_w)]
        above = fixed.at[c, z_rows(1), pl.ds(half_w, half_w)]
        arrived(14, c, fixed.at[c, z_rows(3)])
        start(16, c, below, below, z_up)
        arrived(15, c, fixed.at[c, z_rows(1)])
        start(17, c, above, above, z_down)

    def stage_back(c):
        p, h, cols = where(c)
        arrived(16, c, fixed.at[c, z_rows(2), pl.ds(0, half_w)])
        arrived(17, c, fixed.at[c, z_rows(2), pl.ds(half_w, half_w)])
        values = split(fixed[c])
        for r in range(4):
            back[p, r] += dot3(split(tbl[p, r, :, cols]), values, ((1,), (1,)))

    def ends(c):
        p = lax.div(c, per)
        return p, c - p * per == per - 1

    def stage_ret(c):
        p, last = ends(c)

        @pl.when(last)
        def _():
            start_p(0, p, back.at[p, 3, top], ret1.at[p, 0], y_up)
            start_p(1, p, back.at[p, 3, bottom], ret1.at[p, 1], y_down)

    def stage_ret_fold(c):
        p, last = ends(c)

        @pl.when(last)
        def _():
            arrived_p(0, p, ret1.at[p, 0])
            back[p, 2, top] += ret1[p, 0]
            start_p(2, p, back.at[p, 2], ret2.at[p, 0], y_up)
            arrived_p(1, p, ret1.at[p, 1])
            back[p, 1, bottom] += ret1[p, 1]
            start_p(3, p, back.at[p, 1], ret2.at[p, 1], y_down)

    def stage_ret_sum(c):
        p, last = ends(c)

        @pl.when(last)
        def _():
            arrived_p(2, p, ret2.at[p, 0])
            arrived_p(3, p, ret2.at[p, 1])
            back[p, 0] += ret2[p, 0] + ret2[p, 1]

    def coef_send(p):
        source = spec.at[0] if p == 0 else coef.at[p, 0]
        start_p(4, p, source, coef.at[p, 1], y_up)
        start_p(5, p, source, coef.at[p, 2], y_down)

    def coef_relay(p):
        arrived_p(4, p, coef.at[p, 1])
        start_p(6, p, coef.at[p, 1, top], coef.at[p, 3, top], y_up)
        arrived_p(5, p, coef.at[p, 2])
        start_p(7, p, coef.at[p, 2, bottom], coef.at[p, 3, bottom], y_down)

    for p in range(3):
        pltpu.make_async_copy(
            tables.at[p, :, pl.ds(aligned(y * span, WIDTH), span)], tbl.at[p, 0], own_sem.at[0, p]).start()
        pltpu.make_async_copy(spec.at[p], coef.at[p, 0], own_sem.at[1, p]).start()

    peers = (y_up, y_down, z_up, z_down, x_peer, x_near, core)
    barrier = pltpu.get_barrier_semaphore()
    for peer in peers:
        pl.semaphore_signal(barrier, inc=1, device_id=peer, device_id_type=pl.DeviceIdType.MESH)
    pl.semaphore_wait(barrier, len(peers))

    stage_send(0)
    coef_send(0)
    for c in range(1, LEAD):
        stage_send(c)
    for p in range(3):
        pltpu.make_async_copy(coef.at[p, 0], coef.at[p, 0], own_sem.at[1, p]).wait()
    ee, bb = coef[1, 0], coef[2, 0]
    coef[1, 0] = ee + bb
    coef[2, 0] = ee - bb
    back[...] = jnp.zeros_like(back)

    stages = dict(send=stage_send, relay=stage_relay, share=stage_share, pass_on=stage_pass_on,
                  fold=stage_fold, total=stage_total, scale=stage_scale, spread=stage_spread,
                  corr=stage_corr, back=stage_back, ret=stage_ret,
                  ret_fold=stage_ret_fold, ret_sum=stage_ret_sum)

    def tick(t, carry):
        for name in ORDER:
            c = t - DELAY[name]

            @pl.when((c >= 0 if name != "send" else c >= LEAD) & (c < chunks))
            def _():
                stages[name](c)

            if name == "send":
                for p in range(3):
                    if p:
                        @pl.when(t == p * per - 4)
                        def _():
                            coef_send(p)

                    @pl.when(t == (p * per - 2 if p else FIRST))
                    def _():
                        coef_relay(p)

        return carry

    lax.fori_loop(0, chunks + max(DELAY.values()), tick, 0)

    out[0] = back[0, 0]
    out[1] = 0.5 * (back[1, 0] + back[2, 0])
    out[2] = 0.5 * (back[1, 0] - back[2, 0])

    def drain(i, carry):
        def sent(kind, ref):
            pltpu.make_async_copy(ref, ref, send.at[kind, i]).wait()

        quarter_block = tbl.at[0, 0, pl.ds(0, quarter), pl.ds(0, WIDTH)]
        eighth_block = tbl.at[0, 0, pl.ds(0, eighth), pl.ds(0, WIDTH)]
        three_blocks = tbl.at[0, others, pl.ds(0, quarter), pl.ds(0, WIDTH)]
        group_block = fixed.at[0, pl.ds(0, group)]
        half_block = fixed.at[0, pl.ds(0, group), pl.ds(0, half_w)]
        shapes = ([quarter_block] * 2 + [eighth_block] * 4 + [three_blocks] * 3
                  + [half_block] * 2 + [group_block] * 5 + [half_block] * 2)
        for kind, ref in enumerate(shapes):
            sent(kind, ref)
        return carry

    lax.fori_loop(0, SLOTS, drain, 0)

    def drain_p(p, carry):
        sent_p(0, p, ret1.at[p, 0])
        sent_p(1, p, ret1.at[p, 1])
        sent_p(2, p, ret2.at[p, 0])
        sent_p(3, p, ret2.at[p, 1])
        sent_p(4, p, coef.at[p, 1])
        sent_p(5, p, coef.at[p, 2])
        sent_p(6, p, coef.at[p, 3, top])
        sent_p(7, p, coef.at[p, 3, bottom])
        return carry

    lax.fori_loop(0, 3, drain_p, 0)


def local(spectra, tables, apodization, inv_mask, weights):
    _, depth, angles = tables.shape
    nsim = spectra.shape[2]
    span, group = angles // 4, nsim // 4
    chunks = 3 * span // WIDTH
    rows = [v.reshape(1, -1) for v in (weights, apodization, inv_mask)]
    vmem = pl.BlockSpec(memory_space=pltpu.VMEM)
    hbm = pl.BlockSpec(memory_space=pl.ANY)

    def buffer(*shape):
        return pltpu.VMEM(shape, F32)

    return pl.pallas_call(
        kernel,
        out_shape=jax.ShapeDtypeStruct(spectra.shape, F32),
        in_specs=[hbm, hbm, vmem, vmem, vmem],
        out_specs=vmem,
        scratch_shapes=[
            buffer(3, 4, depth, span),
            buffer(2, chunks, depth // 8, WIDTH),
            buffer(3, 4, depth, nsim),
            pltpu.VMEM((4, nsim, depth), BF16),
            pltpu.VMEM((4, nsim, depth), BF16),
            buffer(chunks, nsim, WIDTH),
            buffer(chunks, 2, group, WIDTH // 2),
            buffer(chunks, 2, group, WIDTH),
            buffer(chunks, group, WIDTH),
            buffer(chunks, group, WIDTH),
            buffer(chunks, nsim, WIDTH),
            buffer(3, 4, depth, nsim),
            buffer(3, 2, depth // 2, nsim),
            buffer(3, 2, depth, nsim),
            pltpu.SemaphoreType.DMA((2, 3)),
            pltpu.SemaphoreType.DMA((18, SLOTS)),
            pltpu.SemaphoreType.DMA((18, chunks)),
            pltpu.SemaphoreType.DMA((8, 3)),
            pltpu.SemaphoreType.DMA((8, 3)),
        ],
        compiler_params=pltpu.CompilerParams(
            collective_id=0, has_side_effects=True, vmem_limit_bytes=60 * 1024 * 1024),
    )(spectra, tables, *rows)


def solution(mesh):
    placed = (P(None, "ell", "sims"), P(None, "ell", None), P(), P(), P())
    return jax.shard_map(
        local, mesh=mesh, in_specs=placed, out_specs=P(None, "ell", "sims"), check_vma=False
    )
```

```python
import jax
import jax.numpy as jnp
from jax import lax
from jax.experimental import pallas as pl
from jax.experimental.pallas import tpu as pltpu
from jax.sharding import PartitionSpec as P

WIDTH = 256
SLOTS = 4
ORDER = (
    "share", "back", "cross", "spread", "corr", "ret_fold", "fold", "total", "relay",
    "ret_sum", "pass_on", "ret", "send", "scale",
)
LEAD, FIRST, DIRECT = 2, 1, 3
DELAY = dict(
    relay=0, share=2, pass_on=3, corr=4, fold=5, total=6, cross=8, scale=9, spread=11,
    back=13, ret=13, ret_fold=15, ret_sum=17, send=-2,
)
F32, BF16 = jnp.float32, jnp.bfloat16


def split(x):
    high = x.astype(BF16)
    return high, (x - high.astype(F32)).astype(BF16)


def dot3(a, b, dims):
    def dot(u, v):
        return lax.dot_general(u, v, (dims, ((), ())), preferred_element_type=F32)

    return dot(a[0], b[0]) + (dot(a[0], b[1]) + dot(a[1], b[0]))


def kernel(spec, tables, weights, apod, inv_mask, out, tbl, relay, coef, coef_hi, coef_lo, corr,
           near, part, cross, other, tot, fixed, back, ret1, ret2, own_sem, send, recv, p_send, p_recv):
    sims, ell = lax.axis_index("sims"), lax.axis_index("ell")
    y, z, x = lax.rem(ell, 4), lax.rem(lax.div(ell, 4), 4), lax.div(ell, 16)
    depth, nsim = out.shape[1], out.shape[2]
    span = tbl.shape[3]
    per = span // WIDTH
    chunks = 3 * per
    quarter = depth // 4
    group = nsim // 4
    half_w, half_d = WIDTH // 2, depth // 2

    def ring(v, d):
        return lax.rem(v + d, 4)

    def at_y(d):
        return (sims, (x * 4 + z) * 4 + ring(y, d))

    def at_z(d):
        return (sims, (x * 4 + ring(z, d)) * 4 + y)

    y_up, y_down, z_up, z_down = at_y(1), at_y(3), at_z(1), at_z(3)
    flip1 = sims + 1 - 2 * lax.rem(sims, 2)
    flip2 = lax.rem(sims + 2, 4)
    core, x_near = (flip1, ell), (flip2, ell)
    x_far = (flip2, ((1 - x) * 4 + z) * 4 + y)

    def aligned(v, m):
        return pl.multiple_of(v, m)

    def z_rows(d):
        return pl.ds(aligned(ring(z, d) * group, 8), group)

    def start(kind, c, src, dst, device):
        copy = pltpu.make_async_remote_copy(
            src, dst, send.at[kind, lax.rem(c, SLOTS)], recv.at[kind, c],
            device_id=device, device_id_type=pl.DeviceIdType.MESH)

        @pl.when(c >= SLOTS)
        def _():
            copy.wait_send()

        copy.start()

    def arrived(kind, c, ref):
        pltpu.make_async_copy(ref, ref, recv.at[kind, c]).wait()

    def start_p(kind, p, src, dst, device):
        pltpu.make_async_remote_copy(
            src, dst, p_send.at[kind, p], p_recv.at[kind, p],
            device_id=device, device_id_type=pl.DeviceIdType.MESH).start()

    def arrived_p(kind, p, ref):
        pltpu.make_async_copy(ref, ref, p_recv.at[kind, p]).wait()

    def sent_p(kind, p, ref):
        pltpu.make_async_copy(ref, ref, p_send.at[kind, p]).wait()

    def where(c):
        p = lax.div(c, per)
        h = c - p * per
        return p, h, pl.ds(aligned(h * WIDTH, WIDTH), WIDTH)

    q0 = aligned(sims * quarter, 8)
    near_rows = pl.ds(aligned(flip2 * quarter, 8), quarter)
    core_rows = pl.ds(aligned(flip1 * quarter, 8), quarter)
    last_rows = pl.ds(aligned(lax.rem(flip1 + 2, 4) * quarter, 8), quarter)
    others = pl.ds(1, 3)
    left, right = pl.ds(0, half_w), pl.ds(half_w, half_w)
    top, bottom = pl.ds(0, half_d), pl.ds(half_d, half_d)

    def by_kind(c, run):
        direct = lax.rem(c, SLOTS) == DIRECT

        @pl.when(direct)
        def _():
            run(True)

        @pl.when(jnp.logical_not(direct))
        def _():
            run(False)

    def rows_for(direct):
        count = depth // 2 if direct else quarter
        base = aligned(lax.rem(sims, 2) * count, 8) if direct else q0
        half = count // 2
        return (pl.ds(base, count), pl.ds(base, half),
                pl.ds(aligned(base + half, 8), half), pl.ds(0, half))

    def stage_send(c):
        p, h, cols = where(c)

        def source(rows, d):
            return tables.at[p, rows, pl.ds(aligned(ring(y, d) * span + h * WIDTH, WIDTH), WIDTH)]

        def run(direct):
            rows, low, high, held = rows_for(direct)
            start(2, c, source(low, 2), relay.at[0, c, held], y_up)
            start(3, c, source(high, 2), relay.at[1, c, held], y_down)
            start(0, c, source(rows, 1), tbl.at[p, 1, rows, cols], y_up)
            start(1, c, source(rows, 3), tbl.at[p, 2, rows, cols], y_down)

        by_kind(c, run)

    def stage_relay(c):
        p, h, cols = where(c)

        def run(direct):
            rows, low, high, held = rows_for(direct)
            arrived(2, c, relay.at[0, c, held])
            start(4, c, relay.at[0, c, held], tbl.at[p, 3, low, cols], y_up)
            arrived(3, c, relay.at[1, c, held])
            start(5, c, relay.at[1, c, held], tbl.at[p, 3, high, cols], y_down)

        by_kind(c, run)

    def stage_share(c):
        p, h, cols = where(c)

        def run(direct):
            rows, low, high, held = rows_for(direct)
            arrived(0, c, tbl.at[p, 1, rows, cols])
            arrived(1, c, tbl.at[p, 2, rows, cols])
            arrived(4, c, tbl.at[p, 3, low, cols])
            arrived(5, c, tbl.at[p, 3, high, cols])
            block = tbl.at[p, others, rows, cols]
            if not direct:
                start(6, c, block, block, x_near)
            start(7, c, block, block, core)

        by_kind(c, run)

    def stage_pass_on(c):
        p, h, cols = where(c)

        @pl.when(lax.rem(c, SLOTS) != DIRECT)
        def _():
            block = tbl.at[p, others, near_rows, cols]
            arrived(6, c, block)
            start(8, c, block, block, core)

    def stage_corr(c):
        p, h, cols = where(c)

        def run(direct):
            if direct:
                half = pl.ds(aligned(lax.rem(flip1, 2) * half_d, 8), half_d)
                arrived(7, c, tbl.at[p, others, half, cols])
            else:
                arrived(7, c, tbl.at[p, others, core_rows, cols])
                arrived(8, c, tbl.at[p, others, last_rows, cols])

        by_kind(c, run)

        @pl.when(h == 0)
        def _():
            pltpu.make_async_copy(tbl.at[p, 0], tbl.at[p, 0], own_sem.at[0, p]).wait()
            arrived_p(6, p, coef.at[p, 3, top])
            arrived_p(7, p, coef.at[p, 3, bottom])
            for r in range(4):
                coef_hi[r], coef_lo[r] = split(coef[p, r].T)

        total = dot3((coef_hi[0], coef_lo[0]), split(tbl[p, 0, :, cols]), ((1,), (0,)))
        for r in range(1, 4):
            total += dot3((coef_hi[r], coef_lo[r]), split(tbl[p, r, :, cols]), ((1,), (0,)))
        corr[c] = total
        far = z_rows(2)
        start(9, c, corr.at[c, far, pl.ds(0, half_w)], near.at[c, 0], z_up)
        start(10, c, corr.at[c, far, pl.ds(half_w, half_w)], near.at[c, 1], z_down)

    def stage_fold(c):
        up, down = z_rows(1), z_rows(3)
        arrived(9, c, near.at[c, 0])
        corr[c, up, pl.ds(0, half_w)] += near[c, 0]
        start(11, c, corr.at[c, up], part.at[c, 0], z_up)
        arrived(10, c, near.at[c, 1])
        corr[c, down, pl.ds(half_w, half_w)] += near[c, 1]
        start(12, c, corr.at[c, down], part.at[c, 1], z_down)

    def stage_total(c):
        arrived(11, c, part.at[c, 0])
        arrived(12, c, part.at[c, 1])
        tot[c] = corr[c, z_rows(0)] + (part[c, 0] + part[c, 1])
        start(13, c, tot.at[c, :, left], cross.at[c, 0], x_near)
        start(18, c, tot.at[c, :, right], cross.at[c, 1], x_far)

    def stage_cross(c):
        arrived(13, c, cross.at[c, 0])
        start(19, c, cross.at[c, 0], other.at[c, :, left], x_far)
        arrived(18, c, cross.at[c, 1])
        start(20, c, cross.at[c, 1], other.at[c, :, right], x_near)

    def stage_scale(c):
        p, h, cols = where(c)
        arrived(19, c, other.at[c, :, left])
        arrived(20, c, other.at[c, :, right])
        here = pl.ds(aligned(y * span + h * WIDTH, WIDTH), WIDTH)
        factor = weights[:, here] * apod[:, here] * inv_mask[:, here]
        rows = z_rows(0)
        fixed[c, rows] = (tot[c] + other[c]) * factor
        start(14, c, fixed.at[c, rows], fixed.at[c, rows], z_up)
        start(15, c, fixed.at[c, rows], fixed.at[c, rows], z_down)

    def stage_spread(c):
        below = fixed.at[c, z_rows(3), pl.ds(0, half_w)]
        above = fixed.at[c, z_rows(1), pl.ds(half_w, half_w)]
        arrived(14, c, fixed.at[c, z_rows(3)])
        start(16, c, below, below, z_up)
        arrived(15, c, fixed.at[c, z_rows(1)])
        start(17, c, above, above, z_down)

    def stage_back(c):
        p, h, cols = where(c)
        arrived(16, c, fixed.at[c, z_rows(2), pl.ds(0, half_w)])
        arrived(17, c, fixed.at[c, z_rows(2), pl.ds(half_w, half_w)])
        values = split(fixed[c])
        for r in range(4):
            back[p, r] += dot3(split(tbl[p, r, :, cols]), values, ((1,), (1,)))

    def ends(c):
        p = lax.div(c, per)
        return p, c - p * per == per - 1

    def stage_ret(c):
        p, last = ends(c)

        @pl.when(last)
        def _():
            start_p(0, p, back.at[p, 3, top], ret1.at[p, 0], y_up)
            start_p(1, p, back.at[p, 3, bottom], ret1.at[p, 1], y_down)
            start_p(2, p, back.at[p, 2, bottom], ret2.at[p, 0, bottom], y_up)
            start_p(3, p, back.at[p, 1, top], ret2.at[p, 1, top], y_down)

    def stage_ret_fold(c):
        p, last = ends(c)

        @pl.when(last)
        def _():
            arrived_p(0, p, ret1.at[p, 0])
            back[p, 2, top] += ret1[p, 0]
            start_p(8, p, back.at[p, 2, top], ret2.at[p, 0, top], y_up)
            arrived_p(1, p, ret1.at[p, 1])
            back[p, 1, bottom] += ret1[p, 1]
            start_p(9, p, back.at[p, 1, bottom], ret2.at[p, 1, bottom], y_down)

    def stage_ret_sum(c):
        p, last = ends(c)

        @pl.when(last)
        def _():
            arrived_p(2, p, ret2.at[p, 0, bottom])
            arrived_p(3, p, ret2.at[p, 1, top])
            arrived_p(8, p, ret2.at[p, 0, top])
            arrived_p(9, p, ret2.at[p, 1, bottom])
            back[p, 0] += ret2[p, 0] + ret2[p, 1]

    def coef_send(p):
        source = spec.at[0] if p == 0 else coef.at[p, 0]
        start_p(4, p, source, coef.at[p, 1], y_up)
        start_p(5, p, source, coef.at[p, 2], y_down)

    def coef_relay(p):
        arrived_p(4, p, coef.at[p, 1])
        start_p(6, p, coef.at[p, 1, top], coef.at[p, 3, top], y_up)
        arrived_p(5, p, coef.at[p, 2])
        start_p(7, p, coef.at[p, 2, bottom], coef.at[p, 3, bottom], y_down)

    for p in range(3):
        pltpu.make_async_copy(
            tables.at[p, :, pl.ds(aligned(y * span, WIDTH), span)], tbl.at[p, 0], own_sem.at[0, p]).start()
        pltpu.make_async_copy(spec.at[p], coef.at[p, 0], own_sem.at[1, p]).start()

    peers = (y_up, y_down, z_up, z_down, x_far, x_near, core)
    barrier = pltpu.get_barrier_semaphore()
    for peer in peers:
        pl.semaphore_signal(barrier, inc=1, device_id=peer, device_id_type=pl.DeviceIdType.MESH)
    pl.semaphore_wait(barrier, len(peers))

    stage_send(0)
    coef_send(0)
    for c in range(1, LEAD):
        stage_send(c)
    for p in range(3):
        pltpu.make_async_copy(coef.at[p, 0], coef.at[p, 0], own_sem.at[1, p]).wait()
    ee, bb = coef[1, 0], coef[2, 0]
    coef[1, 0] = ee + bb
    coef[2, 0] = ee - bb
    back[...] = jnp.zeros_like(back)

    stages = dict(send=stage_send, relay=stage_relay, share=stage_share, pass_on=stage_pass_on,
                  fold=stage_fold, total=stage_total, cross=stage_cross, scale=stage_scale, spread=stage_spread,
                  corr=stage_corr, back=stage_back, ret=stage_ret,
                  ret_fold=stage_ret_fold, ret_sum=stage_ret_sum)

    def tick(t, carry):
        for name in ORDER:
            c = t - DELAY[name]

            @pl.when((c >= 0 if name != "send" else c >= LEAD) & (c < chunks))
            def _():
                stages[name](c)

            if name == "send":
                for p in range(3):
                    if p:
                        @pl.when(t == p * per - 4)
                        def _():
                            coef_send(p)

                    @pl.when(t == (p * per - 2 if p else FIRST))
                    def _():
                        coef_relay(p)

        return carry

    lax.fori_loop(0, chunks + max(DELAY.values()), tick, 0)

    out[0] = back[0, 0]
    out[1] = 0.5 * (back[1, 0] + back[2, 0])
    out[2] = 0.5 * (back[1, 0] - back[2, 0])

    def block(ref, count, width=WIDTH):
        return ref.at[0, pl.ds(0, count), pl.ds(0, width)]

    for i in range(SLOTS):
        count = depth // 2 if i == DIRECT else quarter
        three = tbl.at[0, others, pl.ds(0, count), pl.ds(0, WIDTH)]
        one, two = block(corr, group), block(corr, group, half_w)
        whole, half = block(tbl.at[0], count), block(tbl.at[0], count // 2)
        shapes = [whole] * 2 + [half] * 4 + [three] * 3 + [two] * 2 + [one] * 2
        shapes += [two] + [one] * 2 + [two] * 5
        for kind, ref in enumerate(shapes):
            if i != DIRECT or kind not in (6, 8):
                pltpu.make_async_copy(ref, ref, send.at[kind, i]).wait()

    def drain_p(p, carry):
        sent_p(0, p, ret1.at[p, 0])
        sent_p(1, p, ret1.at[p, 1])
        sent_p(2, p, ret2.at[p, 0, bottom])
        sent_p(3, p, ret2.at[p, 1, top])
        sent_p(8, p, ret2.at[p, 0, top])
        sent_p(9, p, ret2.at[p, 1, bottom])
        sent_p(4, p, coef.at[p, 1])
        sent_p(5, p, coef.at[p, 2])
        sent_p(6, p, coef.at[p, 3, top])
        sent_p(7, p, coef.at[p, 3, bottom])
        return carry

    lax.fori_loop(0, 3, drain_p, 0)


def local(spectra, tables, apodization, inv_mask, weights):
    _, depth, angles = tables.shape
    nsim = spectra.shape[2]
    span, group = angles // 4, nsim // 4
    chunks = 3 * span // WIDTH
    rows = [v.reshape(1, -1) for v in (weights, apodization, inv_mask)]
    vmem = pl.BlockSpec(memory_space=pltpu.VMEM)
    hbm = pl.BlockSpec(memory_space=pl.ANY)

    def buffer(*shape):
        return pltpu.VMEM(shape, F32)

    return pl.pallas_call(
        kernel,
        out_shape=jax.ShapeDtypeStruct(spectra.shape, F32),
        in_specs=[hbm, hbm, vmem, vmem, vmem],
        out_specs=vmem,
        scratch_shapes=[
            buffer(3, 4, depth, span),
            buffer(2, chunks, depth // 4, WIDTH),
            buffer(3, 4, depth, nsim),
            pltpu.VMEM((4, nsim, depth), BF16),
            pltpu.VMEM((4, nsim, depth), BF16),
            buffer(chunks, nsim, WIDTH),
            buffer(chunks, 2, group, WIDTH // 2),
            buffer(chunks, 2, group, WIDTH),
            buffer(chunks, 2, group, WIDTH // 2),
            buffer(chunks, group, WIDTH),
            buffer(chunks, group, WIDTH),
            buffer(chunks, nsim, WIDTH),
            buffer(3, 4, depth, nsim),
            buffer(3, 2, depth // 2, nsim),
            buffer(3, 2, depth, nsim),
            pltpu.SemaphoreType.DMA((2, 3)),
            pltpu.SemaphoreType.DMA((21, SLOTS)),
            pltpu.SemaphoreType.DMA((21, chunks)),
            pltpu.SemaphoreType.DMA((10, 3)),
            pltpu.SemaphoreType.DMA((10, 3)),
        ],
        compiler_params=pltpu.CompilerParams(
            collective_id=0, has_side_effects=True, vmem_limit_bytes=60 * 1024 * 1024),
    )(spectra, tables, *rows)


def solution(mesh):
    placed = (P(None, "ell", "sims"), P(None, "ell", None), P(), P(), P())
    return jax.shard_map(
        local, mesh=mesh, in_specs=placed, out_specs=P(None, "ell", "sims"), check_vma=False
    )
```

```python
import jax
import jax.numpy as jnp
from jax import lax
from jax.experimental import pallas as pl
from jax.experimental.pallas import tpu as pltpu
from jax.sharding import PartitionSpec as P

WIDTH = 256
SLOTS = 4
ORDER = (
    "share", "back", "cross", "spread", "corr", "ret_fold", "fold", "total", "relay",
    "ret_sum", "pass_on", "ret", "send", "scale",
)
LEAD, FIRST, DIRECT, STRIP_LAG = 2, 1, 3, 2
DELAY = dict(
    relay=0, share=2, pass_on=3, corr=4, fold=5, total=6, cross=8, scale=9, spread=11,
    back=13, ret=13, ret_fold=15, ret_sum=17, send=-2,
)
F32, BF16 = jnp.float32, jnp.bfloat16


def split(x):
    high = x.astype(BF16)
    return high, (x - high.astype(F32)).astype(BF16)


def dot3(a, b, dims):
    def dot(u, v):
        return lax.dot_general(u, v, (dims, ((), ())), preferred_element_type=F32)

    return dot(a[0], b[0]) + (dot(a[0], b[1]) + dot(a[1], b[0]))


def kernel(spec, tables, weights, apod, inv_mask, out, tbl, relay, coef, coef_hi, coef_lo, corr,
           near, part, cross, other, tot, fixed, back, ret1, ret2, own_sem, send, recv, p_send, p_recv,
           s_send, s_recv):
    sims, ell = lax.axis_index("sims"), lax.axis_index("ell")
    y, z, x = lax.rem(ell, 4), lax.rem(lax.div(ell, 4), 4), lax.div(ell, 16)
    depth, nsim = out.shape[1], out.shape[2]
    span = tbl.shape[3]
    per = span // WIDTH
    chunks = 3 * per
    quarter = depth // 4
    group = nsim // 4
    half_w, half_d = WIDTH // 2, depth // 2

    def ring(v, d):
        return lax.rem(v + d, 4)

    def at_y(d):
        return (sims, (x * 4 + z) * 4 + ring(y, d))

    def at_z(d):
        return (sims, (x * 4 + ring(z, d)) * 4 + y)

    y_up, y_down, z_up, z_down = at_y(1), at_y(3), at_z(1), at_z(3)
    flip1 = sims + 1 - 2 * lax.rem(sims, 2)
    flip2 = lax.rem(sims + 2, 4)
    core, x_near = (flip1, ell), (flip2, ell)
    x_far = (flip2, ((1 - x) * 4 + z) * 4 + y)

    def aligned(v, m):
        return pl.multiple_of(v, m)

    def z_rows(d):
        return pl.ds(aligned(ring(z, d) * group, 8), group)

    def start(kind, c, src, dst, device):
        copy = pltpu.make_async_remote_copy(
            src, dst, send.at[kind, lax.rem(c, SLOTS)], recv.at[kind, c],
            device_id=device, device_id_type=pl.DeviceIdType.MESH)

        @pl.when(c >= SLOTS)
        def _():
            copy.wait_send()

        copy.start()

    def arrived(kind, c, ref):
        pltpu.make_async_copy(ref, ref, recv.at[kind, c]).wait()

    def start_p(kind, p, src, dst, device):
        pltpu.make_async_remote_copy(
            src, dst, p_send.at[kind, p], p_recv.at[kind, p],
            device_id=device, device_id_type=pl.DeviceIdType.MESH).start()

    def arrived_p(kind, p, ref):
        pltpu.make_async_copy(ref, ref, p_recv.at[kind, p]).wait()

    def sent_p(kind, p, ref):
        pltpu.make_async_copy(ref, ref, p_send.at[kind, p]).wait()

    def where(c):
        p = lax.div(c, per)
        h = c - p * per
        return p, h, pl.ds(aligned(h * WIDTH, WIDTH), WIDTH)

    q0 = aligned(sims * quarter, 8)
    near_rows = pl.ds(aligned(flip2 * quarter, 8), quarter)
    core_rows = pl.ds(aligned(flip1 * quarter, 8), quarter)
    last_rows = pl.ds(aligned(lax.rem(flip1 + 2, 4) * quarter, 8), quarter)
    others = pl.ds(1, 3)
    left, right = pl.ds(0, half_w), pl.ds(half_w, half_w)
    top, bottom = pl.ds(0, half_d), pl.ds(half_d, half_d)

    def by_kind(c, run):
        direct = lax.rem(c, SLOTS) == DIRECT

        @pl.when(direct)
        def _():
            run(True)

        @pl.when(jnp.logical_not(direct))
        def _():
            run(False)

    def rows_for(direct):
        count = depth // 2 if direct else quarter
        base = aligned(lax.rem(sims, 2) * count, 8) if direct else q0
        half = count // 2
        return (pl.ds(base, count), pl.ds(base, half),
                pl.ds(aligned(base + half, 8), half), pl.ds(0, half))

    def stage_send(c):
        p, h, cols = where(c)

        def source(rows, d):
            return tables.at[p, rows, pl.ds(aligned(ring(y, d) * span + h * WIDTH, WIDTH), WIDTH)]

        def run(direct):
            rows, low, high, held = rows_for(direct)
            start(2, c, source(low, 2), relay.at[0, c, held], y_up)
            start(3, c, source(high, 2), relay.at[1, c, held], y_down)
            start(0, c, source(rows, 1), tbl.at[p, 1, rows, cols], y_up)
            start(1, c, source(rows, 3), tbl.at[p, 2, rows, cols], y_down)

        by_kind(c, run)

    def stage_relay(c):
        p, h, cols = where(c)

        def run(direct):
            rows, low, high, held = rows_for(direct)
            arrived(2, c, relay.at[0, c, held])
            start(4, c, relay.at[0, c, held], tbl.at[p, 3, low, cols], y_up)
            arrived(3, c, relay.at[1, c, held])
            start(5, c, relay.at[1, c, held], tbl.at[p, 3, high, cols], y_down)

        by_kind(c, run)

    def stage_share(c):
        p, h, cols = where(c)

        def run(direct):
            rows, low, high, held = rows_for(direct)
            arrived(0, c, tbl.at[p, 1, rows, cols])
            arrived(1, c, tbl.at[p, 2, rows, cols])
            arrived(4, c, tbl.at[p, 3, low, cols])
            arrived(5, c, tbl.at[p, 3, high, cols])
            block = tbl.at[p, others, rows, cols]
            if not direct:
                start(6, c, block, block, x_near)
            start(7, c, block, block, core)

        by_kind(c, run)

    def stage_pass_on(c):
        p, h, cols = where(c)

        @pl.when(lax.rem(c, SLOTS) != DIRECT)
        def _():
            block = tbl.at[p, others, near_rows, cols]
            arrived(6, c, block)
            start(8, c, block, block, core)

    def stage_corr(c):
        p, h, cols = where(c)

        def run(direct):
            if direct:
                half = pl.ds(aligned(lax.rem(flip1, 2) * half_d, 8), half_d)
                arrived(7, c, tbl.at[p, others, half, cols])
            else:
                arrived(7, c, tbl.at[p, others, core_rows, cols])
                arrived(8, c, tbl.at[p, others, last_rows, cols])

        by_kind(c, run)

        @pl.when(h == 0)
        def _():
            pltpu.make_async_copy(tbl.at[p, 0], tbl.at[p, 0], own_sem.at[0, p]).wait()
            @pl.when(p == 0)
            def _():
                arrived_p(6, 0, coef.at[0, 3, top])
                arrived_p(7, 0, coef.at[0, 3, bottom])

            @pl.when(p > 0)
            def _():
                for k in range(per):
                    done_s(s_recv, 2, (p - 1) * per + k, coef.at[p, 3, pl.ds(k * strip, strip)])

            for r in range(4):
                coef_hi[r], coef_lo[r] = split(coef[p, r].T)

        total = dot3((coef_hi[0], coef_lo[0]), split(tbl[p, 0, :, cols]), ((1,), (0,)))
        for r in range(1, 4):
            total += dot3((coef_hi[r], coef_lo[r]), split(tbl[p, r, :, cols]), ((1,), (0,)))
        corr[c] = total
        far = z_rows(2)
        start(9, c, corr.at[c, far, pl.ds(0, half_w)], near.at[c, 0], z_up)
        start(10, c, corr.at[c, far, pl.ds(half_w, half_w)], near.at[c, 1], z_down)

    def stage_fold(c):
        up, down = z_rows(1), z_rows(3)
        arrived(9, c, near.at[c, 0])
        corr[c, up, pl.ds(0, half_w)] += near[c, 0]
        start(11, c, corr.at[c, up], part.at[c, 0], z_up)
        arrived(10, c, near.at[c, 1])
        corr[c, down, pl.ds(half_w, half_w)] += near[c, 1]
        start(12, c, corr.at[c, down], part.at[c, 1], z_down)

    def stage_total(c):
        arrived(11, c, part.at[c, 0])
        arrived(12, c, part.at[c, 1])
        tot[c] = corr[c, z_rows(0)] + (part[c, 0] + part[c, 1])
        start(13, c, tot.at[c, :, left], cross.at[c, 0], x_near)
        start(18, c, tot.at[c, :, right], cross.at[c, 1], x_far)

    def stage_cross(c):
        arrived(13, c, cross.at[c, 0])
        start(19, c, cross.at[c, 0], other.at[c, :, left], x_far)
        arrived(18, c, cross.at[c, 1])
        start(20, c, cross.at[c, 1], other.at[c, :, right], x_near)

    def stage_scale(c):
        p, h, cols = where(c)
        arrived(19, c, other.at[c, :, left])
        arrived(20, c, other.at[c, :, right])
        here = pl.ds(aligned(y * span + h * WIDTH, WIDTH), WIDTH)
        factor = weights[:, here] * apod[:, here] * inv_mask[:, here]
        rows = z_rows(0)
        fixed[c, rows] = (tot[c] + other[c]) * factor
        start(14, c, fixed.at[c, rows], fixed.at[c, rows], z_up)
        start(15, c, fixed.at[c, rows], fixed.at[c, rows], z_down)

    def stage_spread(c):
        below = fixed.at[c, z_rows(3), pl.ds(0, half_w)]
        above = fixed.at[c, z_rows(1), pl.ds(half_w, half_w)]
        arrived(14, c, fixed.at[c, z_rows(3)])
        start(16, c, below, below, z_up)
        arrived(15, c, fixed.at[c, z_rows(1)])
        start(17, c, above, above, z_down)

    def stage_back(c):
        p, h, cols = where(c)
        arrived(16, c, fixed.at[c, z_rows(2), pl.ds(0, half_w)])
        arrived(17, c, fixed.at[c, z_rows(2), pl.ds(half_w, half_w)])
        values = split(fixed[c])
        for r in range(4):
            back[p, r] += dot3(split(tbl[p, r, :, cols]), values, ((1,), (1,)))

    def ends(c):
        p = lax.div(c, per)
        return p, c - p * per == per - 1

    def stage_ret(c):
        p, last = ends(c)

        @pl.when(last)
        def _():
            start_p(0, p, back.at[p, 3, top], ret1.at[p, 0], y_up)
            start_p(1, p, back.at[p, 3, bottom], ret1.at[p, 1], y_down)
            start_p(2, p, back.at[p, 2, bottom], ret2.at[p, 0, bottom], y_up)
            start_p(3, p, back.at[p, 1, top], ret2.at[p, 1, top], y_down)

    def stage_ret_fold(c):
        p, last = ends(c)

        @pl.when(last)
        def _():
            arrived_p(0, p, ret1.at[p, 0])
            back[p, 2, top] += ret1[p, 0]
            start_p(8, p, back.at[p, 2, top], ret2.at[p, 0, top], y_up)
            arrived_p(1, p, ret1.at[p, 1])
            back[p, 1, bottom] += ret1[p, 1]
            start_p(9, p, back.at[p, 1, bottom], ret2.at[p, 1, bottom], y_down)

    def stage_ret_sum(c):
        p, last = ends(c)

        @pl.when(last)
        def _():
            arrived_p(2, p, ret2.at[p, 0, bottom])
            arrived_p(3, p, ret2.at[p, 1, top])
            arrived_p(8, p, ret2.at[p, 0, top])
            arrived_p(9, p, ret2.at[p, 1, bottom])
            back[p, 0] += ret2[p, 0] + ret2[p, 1]

    def coef_send():
        start_p(4, 0, spec.at[0], coef.at[0, 1], y_up)
        start_p(5, 0, spec.at[0], coef.at[0, 2], y_down)

    def coef_relay():
        arrived_p(4, 0, coef.at[0, 1])
        start_p(6, 0, coef.at[0, 1, top], coef.at[0, 3, top], y_up)
        arrived_p(5, 0, coef.at[0, 2])
        start_p(7, 0, coef.at[0, 2, bottom], coef.at[0, 3, bottom], y_down)

    strip = depth // per

    def strip_of(i):
        p, k = lax.div(i, per), lax.rem(i, per)
        return p + 1, k, pl.ds(aligned(k * strip, 8), strip)

    def start_s(kind, i, src, dst, device):
        pltpu.make_async_remote_copy(
            src, dst, s_send.at[kind, i], s_recv.at[kind, i],
            device_id=device, device_id_type=pl.DeviceIdType.MESH).start()

    def done_s(sems, kind, i, ref):
        pltpu.make_async_copy(ref, ref, sems.at[kind, i]).wait()

    def strip_send(i):
        p, k, rows = strip_of(i)
        start_s(0, i, coef.at[p, 0, rows], coef.at[p, 1, rows], y_up)
        start_s(1, i, coef.at[p, 0, rows], coef.at[p, 2, rows], y_down)

    def strip_relay(i):
        p, k, rows = strip_of(i)
        done_s(s_recv, 0, i, coef.at[p, 1, rows])
        done_s(s_recv, 1, i, coef.at[p, 2, rows])

        @pl.when(k < per // 2)
        def _():
            start_s(2, i, coef.at[p, 1, rows], coef.at[p, 3, rows], y_up)

        @pl.when(k >= per // 2)
        def _():
            start_s(2, i, coef.at[p, 2, rows], coef.at[p, 3, rows], y_down)

    for p in range(3):
        pltpu.make_async_copy(
            tables.at[p, :, pl.ds(aligned(y * span, WIDTH), span)], tbl.at[p, 0], own_sem.at[0, p]).start()
        pltpu.make_async_copy(spec.at[p], coef.at[p, 0], own_sem.at[1, p]).start()

    peers = (y_up, y_down, z_up, z_down, x_far, x_near, core)
    barrier = pltpu.get_barrier_semaphore()
    for peer in peers:
        pl.semaphore_signal(barrier, inc=1, device_id=peer, device_id_type=pl.DeviceIdType.MESH)
    pl.semaphore_wait(barrier, len(peers))

    stage_send(0)
    coef_send()
    for c in range(1, LEAD):
        stage_send(c)
    for p in range(3):
        pltpu.make_async_copy(coef.at[p, 0], coef.at[p, 0], own_sem.at[1, p]).wait()
    ee, bb = coef[1, 0], coef[2, 0]
    coef[1, 0] = ee + bb
    coef[2, 0] = ee - bb
    back[...] = jnp.zeros_like(back)

    stages = dict(send=stage_send, relay=stage_relay, share=stage_share, pass_on=stage_pass_on,
                  fold=stage_fold, total=stage_total, cross=stage_cross, scale=stage_scale, spread=stage_spread,
                  corr=stage_corr, back=stage_back, ret=stage_ret,
                  ret_fold=stage_ret_fold, ret_sum=stage_ret_sum)

    def tick(t, carry):
        for name in ORDER:
            c = t - DELAY[name]

            @pl.when((c >= 0 if name != "send" else c >= LEAD) & (c < chunks))
            def _():
                stages[name](c)

            if name == "send":
                @pl.when(t == FIRST)
                def _():
                    coef_relay()

                @pl.when(t < 2 * per)
                def _():
                    strip_send(t)

                @pl.when((t >= STRIP_LAG) & (t < 2 * per + STRIP_LAG))
                def _():
                    strip_relay(t - STRIP_LAG)

        return carry

    lax.fori_loop(0, chunks + max(DELAY.values()), tick, 0)

    out[0] = back[0, 0]
    out[1] = 0.5 * (back[1, 0] + back[2, 0])
    out[2] = 0.5 * (back[1, 0] - back[2, 0])

    def block(ref, count, width=WIDTH):
        return ref.at[0, pl.ds(0, count), pl.ds(0, width)]

    for i in range(SLOTS):
        count = depth // 2 if i == DIRECT else quarter
        three = tbl.at[0, others, pl.ds(0, count), pl.ds(0, WIDTH)]
        one, two = block(corr, group), block(corr, group, half_w)
        whole, half = block(tbl.at[0], count), block(tbl.at[0], count // 2)
        shapes = [whole] * 2 + [half] * 4 + [three] * 3 + [two] * 2 + [one] * 2
        shapes += [two] + [one] * 2 + [two] * 5
        for kind, ref in enumerate(shapes):
            if i != DIRECT or kind not in (6, 8):
                pltpu.make_async_copy(ref, ref, send.at[kind, i]).wait()

    def drain_p(p, carry):
        sent_p(0, p, ret1.at[p, 0])
        sent_p(1, p, ret1.at[p, 1])
        sent_p(2, p, ret2.at[p, 0, bottom])
        sent_p(3, p, ret2.at[p, 1, top])
        sent_p(8, p, ret2.at[p, 0, top])
        sent_p(9, p, ret2.at[p, 1, bottom])
        return carry

    lax.fori_loop(0, 3, drain_p, 0)
    sent_p(4, 0, coef.at[0, 1])
    sent_p(5, 0, coef.at[0, 2])
    sent_p(6, 0, coef.at[0, 3, top])
    sent_p(7, 0, coef.at[0, 3, bottom])

    def drain_s(i, carry):
        for kind in range(3):
            done_s(s_send, kind, i, coef.at[1, kind, pl.ds(0, strip)])
        return carry

    lax.fori_loop(0, 2 * per, drain_s, 0)


def local(spectra, tables, apodization, inv_mask, weights):
    _, depth, angles = tables.shape
    nsim = spectra.shape[2]
    span, group = angles // 4, nsim // 4
    chunks = 3 * span // WIDTH
    rows = [v.reshape(1, -1) for v in (weights, apodization, inv_mask)]
    vmem = pl.BlockSpec(memory_space=pltpu.VMEM)
    hbm = pl.BlockSpec(memory_space=pl.ANY)

    def buffer(*shape):
        return pltpu.VMEM(shape, F32)

    return pl.pallas_call(
        kernel,
        out_shape=jax.ShapeDtypeStruct(spectra.shape, F32),
        in_specs=[hbm, hbm, vmem, vmem, vmem],
        out_specs=vmem,
        scratch_shapes=[
            buffer(3, 4, depth, span),
            buffer(2, chunks, depth // 4, WIDTH),
            buffer(3, 4, depth, nsim),
            pltpu.VMEM((4, nsim, depth), BF16),
            pltpu.VMEM((4, nsim, depth), BF16),
            buffer(chunks, nsim, WIDTH),
            buffer(chunks, 2, group, WIDTH // 2),
            buffer(chunks, 2, group, WIDTH),
            buffer(chunks, 2, group, WIDTH // 2),
            buffer(chunks, group, WIDTH),
            buffer(chunks, group, WIDTH),
            buffer(chunks, nsim, WIDTH),
            buffer(3, 4, depth, nsim),
            buffer(3, 2, depth // 2, nsim),
            buffer(3, 2, depth, nsim),
            pltpu.SemaphoreType.DMA((2, 3)),
            pltpu.SemaphoreType.DMA((21, SLOTS)),
            pltpu.SemaphoreType.DMA((21, chunks)),
            pltpu.SemaphoreType.DMA((10, 3)),
            pltpu.SemaphoreType.DMA((10, 3)),
            pltpu.SemaphoreType.DMA((3, 2 * chunks // 3)),
            pltpu.SemaphoreType.DMA((3, 2 * chunks // 3)),
        ],
        compiler_params=pltpu.CompilerParams(
            collective_id=0, has_side_effects=True, vmem_limit_bytes=60 * 1024 * 1024),
    )(spectra, tables, *rows)


def solution(mesh):
    placed = (P(None, "ell", "sims"), P(None, "ell", None), P(), P(), P())
    return jax.shard_map(
        local, mesh=mesh, in_specs=placed, out_specs=P(None, "ell", "sims"), check_vma=False
    )
```

```python
import jax
import jax.numpy as jnp
from jax import lax
from jax.experimental import pallas as pl
from jax.experimental.pallas import tpu as pltpu
from jax.sharding import PartitionSpec as P

WIDTH = 256
SLOTS = 4
ORDER = (
    "share", "back", "cross", "spread", "corr", "ret_fold", "fold", "total", "relay",
    "ret_sum", "pass_on", "ret", "send", "scale",
)
LEAD, FIRST, DIRECT, STRIP_LAG = 3, 1, 3, 2
DELAY = dict(
    relay=0, share=2, pass_on=3, corr=4, fold=5, total=6, cross=8, scale=9, spread=11,
    back=13, ret=13, ret_fold=15, ret_sum=17, send=-3,
)
F32, BF16 = jnp.float32, jnp.bfloat16


def split(x):
    high = x.astype(BF16)
    return high, (x - high.astype(F32)).astype(BF16)


def dot3(a, b, dims):
    def dot(u, v):
        return lax.dot_general(u, v, (dims, ((), ())), preferred_element_type=F32)

    return dot(a[0], b[0]) + (dot(a[0], b[1]) + dot(a[1], b[0]))


def kernel(spec, tables, weights, apod, inv_mask, out, tbl, relay, coef, coef_hi, coef_lo, corr,
           near, part, cross, other, tot, fixed, back, ret1, ret2, own_sem, send, recv, p_send, p_recv,
           s_send, s_recv):
    sims, ell = lax.axis_index("sims"), lax.axis_index("ell")
    y, z, x = lax.rem(ell, 4), lax.rem(lax.div(ell, 4), 4), lax.div(ell, 16)
    depth, nsim = out.shape[1], out.shape[2]
    span = tbl.shape[3]
    per = span // WIDTH
    chunks = 3 * per
    quarter = depth // 4
    group = nsim // 4
    half_w, half_d = WIDTH // 2, depth // 2

    def ring(v, d):
        return lax.rem(v + d, 4)

    def at_y(d):
        return (sims, (x * 4 + z) * 4 + ring(y, d))

    def at_z(d):
        return (sims, (x * 4 + ring(z, d)) * 4 + y)

    y_up, y_down, z_up, z_down = at_y(1), at_y(3), at_z(1), at_z(3)
    flip1 = sims + 1 - 2 * lax.rem(sims, 2)
    flip2 = lax.rem(sims + 2, 4)
    core, x_near = (flip1, ell), (flip2, ell)
    x_far = (flip2, ((1 - x) * 4 + z) * 4 + y)

    def aligned(v, m):
        return pl.multiple_of(v, m)

    def z_rows(d):
        return pl.ds(aligned(ring(z, d) * group, 8), group)

    def start(kind, c, src, dst, device):
        copy = pltpu.make_async_remote_copy(
            src, dst, send.at[kind, lax.rem(c, SLOTS)], recv.at[kind, c],
            device_id=device, device_id_type=pl.DeviceIdType.MESH)

        @pl.when(c >= SLOTS)
        def _():
            copy.wait_send()

        copy.start()

    def arrived(kind, c, ref):
        pltpu.make_async_copy(ref, ref, recv.at[kind, c]).wait()

    def start_p(kind, p, src, dst, device):
        pltpu.make_async_remote_copy(
            src, dst, p_send.at[kind, p], p_recv.at[kind, p],
            device_id=device, device_id_type=pl.DeviceIdType.MESH).start()

    def arrived_p(kind, p, ref):
        pltpu.make_async_copy(ref, ref, p_recv.at[kind, p]).wait()

    def sent_p(kind, p, ref):
        pltpu.make_async_copy(ref, ref, p_send.at[kind, p]).wait()

    def where(c):
        p = lax.div(c, per)
        h = c - p * per
        return p, h, pl.ds(aligned(h * WIDTH, WIDTH), WIDTH)

    q0 = aligned(sims * quarter, 8)
    near_rows = pl.ds(aligned(flip2 * quarter, 8), quarter)
    core_rows = pl.ds(aligned(flip1 * quarter, 8), quarter)
    last_rows = pl.ds(aligned(lax.rem(flip1 + 2, 4) * quarter, 8), quarter)
    others = pl.ds(1, 3)
    left, right = pl.ds(0, half_w), pl.ds(half_w, half_w)
    top, bottom = pl.ds(0, half_d), pl.ds(half_d, half_d)

    def by_kind(c, run):
        direct = lax.rem(c, SLOTS) == DIRECT

        @pl.when(direct)
        def _():
            run(True)

        @pl.when(jnp.logical_not(direct))
        def _():
            run(False)

    def rows_for(direct):
        count = depth // 2 if direct else quarter
        base = aligned(lax.rem(sims, 2) * count, 8) if direct else q0
        half = count // 2
        return (pl.ds(base, count), pl.ds(base, half),
                pl.ds(aligned(base + half, 8), half), pl.ds(0, half))

    def stage_send(c):
        p, h, cols = where(c)

        def source(rows, d):
            return tables.at[p, rows, pl.ds(aligned(ring(y, d) * span + h * WIDTH, WIDTH), WIDTH)]

        def run(direct):
            rows, low, high, held = rows_for(direct)
            start(2, c, source(low, 2), relay.at[0, c, held], y_up)
            start(3, c, source(high, 2), relay.at[1, c, held], y_down)
            start(0, c, source(rows, 1), tbl.at[p, 1, rows, cols], y_up)
            start(1, c, source(rows, 3), tbl.at[p, 2, rows, cols], y_down)

        by_kind(c, run)

    def stage_relay(c):
        p, h, cols = where(c)

        def run(direct):
            rows, low, high, held = rows_for(direct)
            arrived(2, c, relay.at[0, c, held])
            start(4, c, relay.at[0, c, held], tbl.at[p, 3, low, cols], y_up)
            arrived(3, c, relay.at[1, c, held])
            start(5, c, relay.at[1, c, held], tbl.at[p, 3, high, cols], y_down)

        by_kind(c, run)

    def stage_share(c):
        p, h, cols = where(c)

        def run(direct):
            rows, low, high, held = rows_for(direct)
            arrived(0, c, tbl.at[p, 1, rows, cols])
            arrived(1, c, tbl.at[p, 2, rows, cols])
            arrived(4, c, tbl.at[p, 3, low, cols])
            arrived(5, c, tbl.at[p, 3, high, cols])
            block = tbl.at[p, others, rows, cols]
            if not direct:
                start(6, c, block, block, x_near)
            start(7, c, block, block, core)

        by_kind(c, run)

    def stage_pass_on(c):
        p, h, cols = where(c)

        @pl.when(lax.rem(c, SLOTS) != DIRECT)
        def _():
            block = tbl.at[p, others, near_rows, cols]
            arrived(6, c, block)
            start(8, c, block, block, core)

    def stage_corr(c):
        p, h, cols = where(c)

        def run(direct):
            if direct:
                half = pl.ds(aligned(lax.rem(flip1, 2) * half_d, 8), half_d)
                arrived(7, c, tbl.at[p, others, half, cols])
            else:
                arrived(7, c, tbl.at[p, others, core_rows, cols])
                arrived(8, c, tbl.at[p, others, last_rows, cols])

        by_kind(c, run)

        @pl.when(h == 0)
        def _():
            pltpu.make_async_copy(tbl.at[p, 0], tbl.at[p, 0], own_sem.at[0, p]).wait()
            @pl.when(p == 0)
            def _():
                arrived_p(6, 0, coef.at[0, 3, top])
                arrived_p(7, 0, coef.at[0, 3, bottom])

            @pl.when(p > 0)
            def _():
                for k in range(per):
                    done_s(s_recv, 2, (p - 1) * per + k, coef.at[p, 3, pl.ds(k * strip, strip)])

            for r in range(4):
                coef_hi[r], coef_lo[r] = split(coef[p, r].T)

        total = dot3((coef_hi[0], coef_lo[0]), split(tbl[p, 0, :, cols]), ((1,), (0,)))
        for r in range(1, 4):
            total += dot3((coef_hi[r], coef_lo[r]), split(tbl[p, r, :, cols]), ((1,), (0,)))
        corr[c] = total
        far = z_rows(2)
        start(9, c, corr.at[c, far, pl.ds(0, half_w)], near.at[c, 0], z_up)
        start(10, c, corr.at[c, far, pl.ds(half_w, half_w)], near.at[c, 1], z_down)

    def stage_fold(c):
        up, down = z_rows(1), z_rows(3)
        arrived(9, c, near.at[c, 0])
        corr[c, up, pl.ds(0, half_w)] += near[c, 0]
        start(11, c, corr.at[c, up], part.at[c, 0], z_up)
        arrived(10, c, near.at[c, 1])
        corr[c, down, pl.ds(half_w, half_w)] += near[c, 1]
        start(12, c, corr.at[c, down], part.at[c, 1], z_down)

    def stage_total(c):
        arrived(11, c, part.at[c, 0])
        arrived(12, c, part.at[c, 1])
        tot[c] = corr[c, z_rows(0)] + (part[c, 0] + part[c, 1])
        start(13, c, tot.at[c, :, left], cross.at[c, 0], x_near)
        start(18, c, tot.at[c, :, right], cross.at[c, 1], x_far)

    def stage_cross(c):
        arrived(13, c, cross.at[c, 0])
        start(19, c, cross.at[c, 0], other.at[c, :, left], x_far)
        arrived(18, c, cross.at[c, 1])
        start(20, c, cross.at[c, 1], other.at[c, :, right], x_near)

    def stage_scale(c):
        p, h, cols = where(c)
        arrived(19, c, other.at[c, :, left])
        arrived(20, c, other.at[c, :, right])
        here = pl.ds(aligned(y * span + h * WIDTH, WIDTH), WIDTH)
        factor = weights[:, here] * apod[:, here] * inv_mask[:, here]
        rows = z_rows(0)
        fixed[c, rows] = (tot[c] + other[c]) * factor
        start(14, c, fixed.at[c, rows], fixed.at[c, rows], z_up)
        start(15, c, fixed.at[c, rows], fixed.at[c, rows], z_down)

    def stage_spread(c):
        below = fixed.at[c, z_rows(3), pl.ds(0, half_w)]
        above = fixed.at[c, z_rows(1), pl.ds(half_w, half_w)]
        arrived(14, c, fixed.at[c, z_rows(3)])
        start(16, c, below, below, z_up)
        arrived(15, c, fixed.at[c, z_rows(1)])
        start(17, c, above, above, z_down)

    def stage_back(c):
        p, h, cols = where(c)
        arrived(16, c, fixed.at[c, z_rows(2), pl.ds(0, half_w)])
        arrived(17, c, fixed.at[c, z_rows(2), pl.ds(half_w, half_w)])
        values = split(fixed[c])
        for r in range(4):
            back[p, r] += dot3(split(tbl[p, r, :, cols]), values, ((1,), (1,)))

    def ends(c):
        p = lax.div(c, per)
        return p, c - p * per == per - 1

    def stage_ret(c):
        p, last = ends(c)

        @pl.when(last)
        def _():
            start_p(0, p, back.at[p, 3, top], ret1.at[p, 0], y_up)
            start_p(1, p, back.at[p, 3, bottom], ret1.at[p, 1], y_down)
            start_p(2, p, back.at[p, 2, bottom], ret2.at[p, 0, bottom], y_up)
            start_p(3, p, back.at[p, 1, top], ret2.at[p, 1, top], y_down)

    def stage_ret_fold(c):
        p, last = ends(c)

        @pl.when(last)
        def _():
            arrived_p(0, p, ret1.at[p, 0])
            back[p, 2, top] += ret1[p, 0]
            start_p(8, p, back.at[p, 2, top], ret2.at[p, 0, top], y_up)
            arrived_p(1, p, ret1.at[p, 1])
            back[p, 1, bottom] += ret1[p, 1]
            start_p(9, p, back.at[p, 1, bottom], ret2.at[p, 1, bottom], y_down)

    def stage_ret_sum(c):
        p, last = ends(c)

        @pl.when(last)
        def _():
            arrived_p(2, p, ret2.at[p, 0, bottom])
            arrived_p(3, p, ret2.at[p, 1, top])
            arrived_p(8, p, ret2.at[p, 0, top])
            arrived_p(9, p, ret2.at[p, 1, bottom])
            back[p, 0] += ret2[p, 0] + ret2[p, 1]

    def coef_send():
        start_p(4, 0, spec.at[0], coef.at[0, 1], y_up)
        start_p(5, 0, spec.at[0], coef.at[0, 2], y_down)

    def coef_relay():
        arrived_p(4, 0, coef.at[0, 1])
        start_p(6, 0, coef.at[0, 1, top], coef.at[0, 3, top], y_up)
        arrived_p(5, 0, coef.at[0, 2])
        start_p(7, 0, coef.at[0, 2, bottom], coef.at[0, 3, bottom], y_down)

    strip = depth // per

    def strip_of(i):
        p, k = lax.div(i, per), lax.rem(i, per)
        return p + 1, k, pl.ds(aligned(k * strip, 8), strip)

    def start_s(kind, i, src, dst, device):
        pltpu.make_async_remote_copy(
            src, dst, s_send.at[kind, i], s_recv.at[kind, i],
            device_id=device, device_id_type=pl.DeviceIdType.MESH).start()

    def done_s(sems, kind, i, ref):
        pltpu.make_async_copy(ref, ref, sems.at[kind, i]).wait()

    def strip_send(i):
        p, k, rows = strip_of(i)
        start_s(0, i, coef.at[p, 0, rows], coef.at[p, 1, rows], y_up)
        start_s(1, i, coef.at[p, 0, rows], coef.at[p, 2, rows], y_down)

    def strip_relay(i):
        p, k, rows = strip_of(i)
        done_s(s_recv, 0, i, coef.at[p, 1, rows])
        done_s(s_recv, 1, i, coef.at[p, 2, rows])

        @pl.when(k < per // 2)
        def _():
            start_s(2, i, coef.at[p, 1, rows], coef.at[p, 3, rows], y_up)

        @pl.when(k >= per // 2)
        def _():
            start_s(2, i, coef.at[p, 2, rows], coef.at[p, 3, rows], y_down)

    for p in range(3):
        pltpu.make_async_copy(
            tables.at[p, :, pl.ds(aligned(y * span, WIDTH), span)], tbl.at[p, 0], own_sem.at[0, p]).start()
        pltpu.make_async_copy(spec.at[p], coef.at[p, 0], own_sem.at[1, p]).start()

    peers = (y_up, y_down, z_up, z_down, x_far, x_near, core)
    barrier = pltpu.get_barrier_semaphore()
    for peer in peers:
        pl.semaphore_signal(barrier, inc=1, device_id=peer, device_id_type=pl.DeviceIdType.MESH)
    pl.semaphore_wait(barrier, len(peers))

    stage_send(0)
    coef_send()
    for c in range(1, LEAD):
        stage_send(c)
    for p in range(3):
        pltpu.make_async_copy(coef.at[p, 0], coef.at[p, 0], own_sem.at[1, p]).wait()
    ee, bb = coef[1, 0], coef[2, 0]
    coef[1, 0] = ee + bb
    coef[2, 0] = ee - bb
    back[...] = jnp.zeros_like(back)

    stages = dict(send=stage_send, relay=stage_relay, share=stage_share, pass_on=stage_pass_on,
                  fold=stage_fold, total=stage_total, cross=stage_cross, scale=stage_scale, spread=stage_spread,
                  corr=stage_corr, back=stage_back, ret=stage_ret,
                  ret_fold=stage_ret_fold, ret_sum=stage_ret_sum)

    def tick(t, carry):
        for name in ORDER:
            c = t - DELAY[name]

            @pl.when((c >= 0 if name != "send" else c >= LEAD) & (c < chunks))
            def _():
                stages[name](c)

            if name == "send":
                @pl.when(t == FIRST)
                def _():
                    coef_relay()

                @pl.when(t < 2 * per)
                def _():
                    strip_send(t)

                @pl.when((t >= STRIP_LAG) & (t < 2 * per + STRIP_LAG))
                def _():
                    strip_relay(t - STRIP_LAG)

        return carry

    lax.fori_loop(0, chunks + max(DELAY.values()), tick, 0)

    out[0] = back[0, 0]
    out[1] = 0.5 * (back[1, 0] + back[2, 0])
    out[2] = 0.5 * (back[1, 0] - back[2, 0])

    def block(ref, count, width=WIDTH):
        return ref.at[0, pl.ds(0, count), pl.ds(0, width)]

    for i in range(SLOTS):
        count = depth // 2 if i == DIRECT else quarter
        three = tbl.at[0, others, pl.ds(0, count), pl.ds(0, WIDTH)]
        one, two = block(corr, group), block(corr, group, half_w)
        whole, half = block(tbl.at[0], count), block(tbl.at[0], count // 2)
        shapes = [whole] * 2 + [half] * 4 + [three] * 3 + [two] * 2 + [one] * 2
        shapes += [two] + [one] * 2 + [two] * 5
        for kind, ref in enumerate(shapes):
            if i != DIRECT or kind not in (6, 8):
                pltpu.make_async_copy(ref, ref, send.at[kind, i]).wait()

    def drain_p(p, carry):
        sent_p(0, p, ret1.at[p, 0])
        sent_p(1, p, ret1.at[p, 1])
        sent_p(2, p, ret2.at[p, 0, bottom])
        sent_p(3, p, ret2.at[p, 1, top])
        sent_p(8, p, ret2.at[p, 0, top])
        sent_p(9, p, ret2.at[p, 1, bottom])
        return carry

    lax.fori_loop(0, 3, drain_p, 0)
    sent_p(4, 0, coef.at[0, 1])
    sent_p(5, 0, coef.at[0, 2])
    sent_p(6, 0, coef.at[0, 3, top])
    sent_p(7, 0, coef.at[0, 3, bottom])

    def drain_s(i, carry):
        for kind in range(3):
            done_s(s_send, kind, i, coef.at[1, kind, pl.ds(0, strip)])
        return carry

    lax.fori_loop(0, 2 * per, drain_s, 0)


def local(spectra, tables, apodization, inv_mask, weights):
    _, depth, angles = tables.shape
    nsim = spectra.shape[2]
    span, group = angles // 4, nsim // 4
    chunks = 3 * span // WIDTH
    rows = [v.reshape(1, -1) for v in (weights, apodization, inv_mask)]
    vmem = pl.BlockSpec(memory_space=pltpu.VMEM)
    hbm = pl.BlockSpec(memory_space=pl.ANY)

    def buffer(*shape):
        return pltpu.VMEM(shape, F32)

    return pl.pallas_call(
        kernel,
        out_shape=jax.ShapeDtypeStruct(spectra.shape, F32),
        in_specs=[hbm, hbm, vmem, vmem, vmem],
        out_specs=vmem,
        scratch_shapes=[
            buffer(3, 4, depth, span),
            buffer(2, chunks, depth // 4, WIDTH),
            buffer(3, 4, depth, nsim),
            pltpu.VMEM((4, nsim, depth), BF16),
            pltpu.VMEM((4, nsim, depth), BF16),
            buffer(chunks, nsim, WIDTH),
            buffer(chunks, 2, group, WIDTH // 2),
            buffer(chunks, 2, group, WIDTH),
            buffer(chunks, 2, group, WIDTH // 2),
            buffer(chunks, group, WIDTH),
            buffer(chunks, group, WIDTH),
            buffer(chunks, nsim, WIDTH),
            buffer(3, 4, depth, nsim),
            buffer(3, 2, depth // 2, nsim),
            buffer(3, 2, depth, nsim),
            pltpu.SemaphoreType.DMA((2, 3)),
            pltpu.SemaphoreType.DMA((21, SLOTS)),
            pltpu.SemaphoreType.DMA((21, chunks)),
            pltpu.SemaphoreType.DMA((10, 3)),
            pltpu.SemaphoreType.DMA((10, 3)),
            pltpu.SemaphoreType.DMA((3, 2 * chunks // 3)),
            pltpu.SemaphoreType.DMA((3, 2 * chunks // 3)),
        ],
        compiler_params=pltpu.CompilerParams(
            collective_id=0, has_side_effects=True, vmem_limit_bytes=60 * 1024 * 1024),
    )(spectra, tables, *rows)


def solution(mesh):
    placed = (P(None, "ell", "sims"), P(None, "ell", None), P(), P(), P())
    return jax.shard_map(
        local, mesh=mesh, in_specs=placed, out_specs=P(None, "ell", "sims"), check_vma=False
    )
```
